32 devices in a mesh: slab: 2 (over x), py: 4 (over y, core), px: 4 (over z).
Axes of the slice: x: 2, y: 2, z: 4, core: 2. Of those that a mesh axis runs over, the one named last changes fastest.
Arguments:
- state: bfloat16 [2, 3, 16, 1024, 1024], P(None, None, 'slab', ('py', 'px')), may hold values from -12 to 12
- shells: int32 [16, 1024, 1024], P('slab', ('py', 'px')), may hold values from 0 to 511
Outputs:
- restored: float32 [2, 3, 16, 1024, 1024], P(None, None, ('slab', 'py'), None, 'px')
- spectrum: float32 [512], replicated
The draws below stay inside these ranges and needn't reach their ends.
All inputs are finite; a program needn't handle non-finite values.
Results may differ from the reference program's by a relative error of at most 0.0003.
Values may be sent and summed in bfloat16 or wider, within the bound.
No kernel may reach another device: no remote copies, remote signals or barrier semaphores. Data moves between devices by JAX's collectives and lax.ppermute only.
A program may use at most 128 MiB of HBM per device.

```python
import math
import jax
import jax.numpy as jnp

X = 1024
Y = 1024
SHELLS = 512
Z = 16


def integer_root(squares):
    root = jnp.zeros_like(squares)
    for level in range(11, -1, -1):
        candidate = root + (1 << level)
        root = jnp.where(candidate * candidate <= squares, candidate, root)
    return root


def centred(count, key):
    spread = count // 8
    centre = count // 2 + jax.random.randint(key, (), -spread, spread + 1, jnp.int32)
    offsets = jnp.arange(count, dtype=jnp.int32) - centre
    reach = jnp.maximum(centre, count - 1 - centre)
    return (offsets, reach)


def shell_labels(key):
    base_key = jax.random.fold_in(key, 29)
    plane_key, row_key, column_key, jitter_key = jax.random.split(base_key, 4)
    plane_off, plane_reach = centred(Z, plane_key)
    row_off, row_reach = centred(Y, row_key)
    column_off, column_reach = centred(X, column_key)
    squares = (plane_off * plane_off)[:, None, None] + (row_off * row_off)[None, :, None] + (column_off * column_off)[None, None, :]
    radius = integer_root(squares)
    outer = integer_root(plane_reach * plane_reach + row_reach * row_reach + column_reach * column_reach)
    labels = radius * SHELLS // (outer + 1)
    jitter = jax.random.randint(jitter_key, (Z, Y, X), 0, 2, jnp.int32)
    return jnp.minimum(labels + jitter, SHELLS - 1).astype(jnp.int32)


def draw_shells(key, part):
    return shell_labels(key)


def draw_state(key, part):
    labels = shell_labels(key)
    first_key = jax.random.fold_in(jax.random.fold_in(key, 11), 0)
    column_key = jax.random.fold_in(jax.random.fold_in(key, 11), 2)
    row_key = jax.random.fold_in(jax.random.fold_in(key, 11), 3)
    decay = 1.0 / jnp.sqrt(1.0 + labels.astype(jnp.float32))
    column_gain = jnp.exp(jax.random.uniform(column_key, (X,), jnp.float32, math.log(0.5), math.log(2.0)))
    row_gain = jnp.exp(jax.random.uniform(row_key, (Y,), jnp.float32, math.log(0.7), math.log(1.4)))
    amplitude = decay * row_gain[None, :, None] * column_gain[None, None, :]
    base = jnp.clip(jax.random.normal(first_key, (2, 3, Z, Y, X), jnp.float32), -4.0, 4.0)
    return (base * amplitude[None, None, :, :, :]).astype(jnp.bfloat16)


def setup_inputs(seed: int = 0) -> dict:
    splits = jax.random.split(jax.random.key(seed), 3)
    state = draw_state(jax.random.fold_in(splits[2], 71), 0)
    shells = draw_shells(jax.random.fold_in(splits[2], 71), 0)
    return {"state": state, "shells": shells}


def reference(state, shells):
    restored = state.astype(jnp.float32)
    energy = 0.5 * jnp.sum(restored * restored, axis=(0, 1))
    totals = jax.ops.segment_sum(energy.reshape(-1), shells.reshape(-1).astype(jnp.int32), num_segments=SHELLS)
    spectrum = totals * (SHELLS / (Z * Y * X))
    return restored, spectrum
```

```python
import functools

import jax
import jax.numpy as jnp
from jax import lax
from jax.experimental import pallas as pl
from jax.experimental.pallas import tpu as pltpu
from jax.sharding import PartitionSpec as P

SHELLS = 512
LOW = 32
HIGH = SHELLS // LOW


def is_power(n):
    return n & (n - 1) == 0


def partner(i, step, n, back=False):
    if is_power(n):
        return i ^ step
    return (i - step + n) % n if back else (i + step) % n


def pack_kernel(steps, sizes, state, *refs):
    (py_n, px_n), n = sizes, len(steps)
    outs, bufs, sem_in, sem_out = refs[:n], refs[n : 2 * n], refs[2 * n], refs[2 * n + 1]
    planes, columns = outs[0].shape[2], outs[0].shape[4]
    me_y, me_x = lax.axis_index("py"), lax.axis_index("px")
    reads, writes = [], []
    for k, (a, b) in enumerate(steps):
        to_y, to_x = partner(me_y, a, py_n), partner(me_x, b, px_n)
        block = state.at[
            :,
            :,
            pl.ds(to_y * planes, planes),
            :,
            pl.ds(pl.multiple_of(to_x * columns, columns), columns),
        ]
        reads.append(pltpu.make_async_copy(block, bufs[k], sem_in.at[k]))
        reads[-1].start()
    for k in range(n):
        reads[k].wait()
        writes.append(pltpu.make_async_copy(bufs[k], outs[k], sem_out.at[k]))
        writes[-1].start()
    for w in writes:
        w.wait()


def pack(state, steps, sizes, piece):
    n = len(steps)
    size = 2 * piece[0] * piece[1] * piece[2] * piece[3] * piece[4]
    return pl.pallas_call(
        functools.partial(pack_kernel, steps, sizes),
        out_shape=[jax.ShapeDtypeStruct(piece, jnp.bfloat16)] * n,
        in_specs=[pl.BlockSpec(memory_space=pltpu.HBM)],
        out_specs=[pl.BlockSpec(memory_space=pl.ANY)] * n,
        scratch_shapes=[pltpu.VMEM(piece, jnp.bfloat16)] * n
        + [pltpu.SemaphoreType.DMA((n,)), pltpu.SemaphoreType.DMA((n,))],
        cost_estimate=pl.CostEstimate(flops=0, bytes_accessed=2 * n * size, transcendentals=0),
        name="pack",
    )(state)


def unpack_kernel(steps, sizes, with_base, with_own, *refs):
    (py_n, px_n), n = sizes, len(steps)
    refs = list(refs)
    if with_base:
        refs.pop(0)
    own = refs.pop(0) if with_own else None
    pieces = [refs.pop(0) for _ in range(n)]
    out, narrow, wide, sem_in, sem_out = refs
    me_y, me_x = lax.axis_index("py"), lax.axis_index("px")
    total = n + (1 if with_own else 0)
    reads, writes = [], []
    for k in range(total):
        if k < n:
            src = pieces[k]
        else:
            planes, columns = narrow.shape[3], narrow.shape[5]
            src = own.at[
                :,
                :,
                pl.ds(me_y * planes, planes),
                :,
                pl.ds(pl.multiple_of(me_x * columns, columns), columns),
            ]
        reads.append(pltpu.make_async_copy(src, narrow.at[k], sem_in.at[k]))
        reads[-1].start()
    for k in range(total):
        a, b = steps[k] if k < n else (0, 0)
        from_y, from_x = partner(me_y, a, py_n, True), partner(me_x, b, px_n, True)
        reads[k].wait()
        wide[k] = narrow[k].astype(jnp.float32)
        writes.append(pltpu.make_async_copy(wide.at[k], out.at[:, :, :, from_y, from_x], sem_out.at[k]))
        writes[-1].start()
    for w in writes:
        w.wait()


def unpack(base, own, pieces, steps, sizes, piece):
    py_n, px_n = sizes
    n = len(steps) + (own is not None)
    shape = piece[:3] + (py_n, px_n) + piece[3:]
    size = piece[0] * piece[1] * piece[2] * piece[3] * piece[4]
    args = ([base] if base is not None else []) + ([own] if own is not None else []) + list(pieces)
    hbm = pl.BlockSpec(memory_space=pltpu.HBM)
    specs = [hbm] * (len(args) - len(pieces)) + [pl.BlockSpec(memory_space=pl.ANY)] * len(pieces)
    return pl.pallas_call(
        functools.partial(unpack_kernel, steps, sizes, base is not None, own is not None),
        out_shape=jax.ShapeDtypeStruct(shape, jnp.float32),
        in_specs=specs,
        out_specs=hbm,
        scratch_shapes=[
            pltpu.VMEM((n,) + piece, jnp.bfloat16),
            pltpu.VMEM((n,) + piece, jnp.float32),
            pltpu.SemaphoreType.DMA((n,)),
            pltpu.SemaphoreType.DMA((n,)),
        ],
        input_output_aliases={0: 0} if base is not None else {},
        cost_estimate=pl.CostEstimate(flops=0, bytes_accessed=6 * n * size, transcendentals=0),
        name="unpack",
    )(*args)


def bin_kernel(state, shells, out):
    rows = 8
    width = shells.shape[2]
    low_ids = lax.broadcasted_iota(jnp.int32, (LOW, width), 0)
    high_ids = lax.broadcasted_iota(jnp.int32, (HIGH, width), 0)

    @pl.when(pl.program_id(0) == 0)
    def _():
        out[...] = jnp.zeros_like(out)

    def body(i, total):
        r0 = pl.multiple_of(i * rows, rows)
        energy = jnp.zeros((rows, width), jnp.float32)
        for c in range(2):
            for d in range(3):
                v = state[c, d, 0, pl.ds(r0, rows), :].astype(jnp.float32)
                energy = energy + v * v
        labels = shells[0, pl.ds(r0, rows), :]
        low, high = labels % LOW, labels // LOW
        upper = energy.astype(jnp.bfloat16).astype(jnp.float32)
        lower = energy - upper
        lhs, rhs = [], []
        for r in range(rows):
            at_low = jnp.broadcast_to(low[r : r + 1], (LOW, width)) == low_ids
            at_high = jnp.broadcast_to(high[r : r + 1], (HIGH, width)) == high_ids
            up = jnp.where(at_high, jnp.broadcast_to(upper[r : r + 1], (HIGH, width)), 0.0)
            lo = jnp.where(at_high, jnp.broadcast_to(lower[r : r + 1], (HIGH, width)), 0.0)
            lhs.append(jnp.concatenate([up.astype(jnp.bfloat16), lo.astype(jnp.bfloat16)], axis=0))
            rhs.append(jnp.where(at_low, 1.0, 0.0).astype(jnp.bfloat16))
        part = lax.dot_general(
            jnp.concatenate(lhs, axis=1),
            jnp.concatenate(rhs, axis=1),
            (((1,), (1,)), ((), ())),
            preferred_element_type=jnp.float32,
        )
        return total + part

    total = lax.fori_loop(0, shells.shape[1] // rows, body, jnp.zeros((2 * HIGH, LOW), jnp.float32))
    out[...] += total[:HIGH] + total[HIGH:]


def bin_energy(state, shells):
    _, _, planes, rows, width = state.shape
    return pl.pallas_call(
        bin_kernel,
        grid=(planes,),
        out_shape=jax.ShapeDtypeStruct((HIGH, LOW), jnp.float32),
        in_specs=[
            pl.BlockSpec((2, 3, 1, rows, width), lambda i: (0, 0, i, 0, 0)),
            pl.BlockSpec((1, rows, width), lambda i: (i, 0, 0)),
        ],
        out_specs=pl.BlockSpec((HIGH, LOW), lambda i: (0, 0)),
        cost_estimate=pl.CostEstimate(
            flops=4 * HIGH * LOW * planes * rows * width,
            bytes_accessed=16 * planes * rows * width,
            transcendentals=0,
        ),
        name="bins",
    )(state, shells)


def local(state, shells):
    py_n, px_n, slab_n = lax.axis_size("py"), lax.axis_size("px"), lax.axis_size("slab")
    sizes = (py_n, px_n)
    _, _, planes, rows, columns = state.shape
    piece = (2, 3, planes // py_n, rows, columns // px_n)

    def send(x, step):
        a, b = step
        pairs = [
            (y * px_n + x_, partner(y, a, py_n) * px_n + partner(x_, b, px_n))
            for y in range(py_n)
            for x_ in range(px_n)
        ]
        return lax.ppermute(x, ("py", "px"), pairs)

    far = [b for b in range(px_n) if b >= px_n // 2]
    near = [b for b in range(px_n) if b < px_n // 2]
    groups = [[(a, b) for a in range(py_n)] for b in reversed(far)]
    groups.append([(a, b) for b in reversed(near) for a in range(py_n) if (a, b) != (0, 0)])
    received = []
    for steps in groups:
        packed = pack(state, steps, sizes, piece)
        received.append([send(x, s) for x, s in zip(packed, steps)])
    totals = bin_energy(state, shells)
    modes = slab_n * py_n * px_n * planes * rows * columns
    totals = lax.psum(totals, ("slab", "py", "px"))
    spectrum = totals.reshape(SHELLS) * (0.5 * SHELLS / modes)
    out = unpack(None, state, [], [], sizes, piece)
    order = [2] + list(range(len(groups) - 1))
    for g in order:
        out = unpack(out, None, received[g], groups[g], sizes, piece)
    restored = out.reshape(2, 3, planes // py_n, py_n * px_n * rows, columns // px_n)
    return (restored, spectrum)


def solution(mesh):
    return jax.shard_map(
        local,
        mesh=mesh,
        in_specs=(P(None, None, "slab", ("py", "px"), None), P("slab", ("py", "px"), None)),
        out_specs=(P(None, None, ("slab", "py"), None, "px"), P()),
        check_vma=False,
    )
```

```python
import functools

import jax
import jax.numpy as jnp
from jax import lax
from jax.experimental import pallas as pl
from jax.experimental.pallas import tpu as pltpu
from jax.sharding import PartitionSpec as P


SHELLS = 512
LOW = 32
HIGH = SHELLS // LOW
LANES = 256
CUTS = (7, 10)
VMEM_LIMIT = 40 * 1024 * 1024
VMEM_FIRST = 56 * 1024 * 1024


def is_power(n):
    return n & (n - 1) == 0


def partner(i, step, n, back=False):
    if is_power(n):
        return i ^ step
    return (i - step + n) % n if back else (i + step) % n


def split3(x):
    a = x.astype(jnp.bfloat16)
    x = x - a.astype(jnp.float32)
    b = x.astype(jnp.bfloat16)
    return a, b, (x - b.astype(jnp.float32)).astype(jnp.bfloat16)


def whole_wait(ref, sem):
    pltpu.make_async_copy(ref, ref, sem).wait()


def pack_kernel(steps, sizes, planes, with_totals, *refs):
    (py_n, px_n), n = sizes, len(steps)
    refs = list(refs)
    state = refs.pop(0)
    totals = refs.pop(0) if with_totals else None
    outs, sems = refs[:n], refs[n]
    rows = state.shape[3]
    columns = outs[0].shape[1]
    me_y, me_x = lax.axis_index("py"), lax.axis_index("px")
    for k, (a, b, first, last, _) in enumerate(steps):
        to_y, to_x = partner(me_y, a, py_n), partner(me_x, b, px_n)
        across = pl.ds(pl.multiple_of(to_x * columns, columns), columns)
        for j in range(first, last):
            c, d, p = j // (3 * planes), j // planes % 3, j % planes
            pltpu.make_async_copy(
                state.at[c, d, to_y * planes + p, :, across],
                outs[k].at[pl.ds((j - first) * rows, rows), :],
                sems.at[k],
            ).start()
    if with_totals:
        t = totals[...]
        terms = split3(t) + (jnp.zeros_like(t).astype(jnp.bfloat16),)
        extra = jnp.concatenate([x.astype(jnp.float32) for x in terms], axis=0).astype(jnp.bfloat16)
        for k, (_, _, first, last, more) in enumerate(steps):
            if more:
                outs[k][pl.ds((last - first) * rows, 8), :] = extra
    for k, (_, _, first, last, _) in enumerate(steps):
        if first < last:
            whole_wait(outs[k].at[pl.ds(0, (last - first) * rows), :], sems.at[k])


def pack(state, totals, steps, sizes, planes):
    rows, columns = state.shape[3], state.shape[4] // sizes[1]
    shapes = [((l - f) * rows + (8 if more else 0), columns) for _, _, f, l, more in steps]
    vmem = pl.BlockSpec(memory_space=pltpu.VMEM)
    return pl.pallas_call(
        functools.partial(pack_kernel, steps, sizes, planes, totals is not None),
        out_shape=[jax.ShapeDtypeStruct(s, jnp.bfloat16) for s in shapes],
        in_specs=[pl.BlockSpec(memory_space=pltpu.HBM)] + ([vmem] if totals is not None else []),
        out_specs=[vmem] * len(steps),
        scratch_shapes=[pltpu.SemaphoreType.DMA((len(steps),))],
        compiler_params=pltpu.CompilerParams(
            vmem_limit_bytes=VMEM_FIRST if totals is None else VMEM_LIMIT
        ),
        cost_estimate=pl.CostEstimate(
            flops=0, bytes_accessed=sum(2 * r * c for r, c in shapes), transcendentals=0
        ),
        name="pack",
    )(state, *([totals] if totals is not None else []))


def unpack_kernel(steps, sizes, planes, with_base, scale, *refs):
    (py_n, px_n), n = sizes, len(steps)
    refs = list(refs)
    if with_base:
        refs.pop(0)
    mine = refs.pop(0) if scale is not None else None
    pieces = [refs.pop(0) for _ in range(n)]
    out = refs.pop(0)
    spectrum = refs.pop(0) if scale is not None else None
    wides, sems = refs[:n], refs[n]
    each = refs[n + 1] if scale is not None else None
    rows = out.shape[5]
    me_y, me_x = lax.axis_index("py"), lax.axis_index("px")
    for k, (a, b, first, last, more) in enumerate(steps):
        from_y, from_x = partner(me_y, a, py_n, True), partner(me_x, b, px_n, True)
        size = (last - first) * rows
        if first < last:
            wides[k][...] = pieces[k][pl.ds(0, size), :].astype(jnp.float32)
        for j in range(first, last):
            c, d, p = j // (3 * planes), j // planes % 3, j % planes
            pltpu.make_async_copy(
                wides[k].at[pl.ds((j - first) * rows, rows), :],
                out.at[c, d, p, from_y, from_x],
                sems.at[k],
            ).start()
        if more:
            extra = pieces[k][pl.ds(size, 8), :].astype(jnp.float32)
            each[from_y * px_n + from_x] = (extra[0:2] + extra[2:4]) + extra[4:6]
    if scale is not None:
        a, b, c = [x.astype(jnp.float32) for x in split3(mine[...])]
        each[me_y * px_n + me_x] = (a + b) + c
        total = each[0]
        for i in range(1, py_n * px_n):
            total = total + each[i]
        spectrum[...] = total * scale
    for k, (_, _, first, last, _) in enumerate(steps):
        if first < last:
            whole_wait(wides[k], sems.at[k])


def unpack(base, mine, pieces, steps, sizes, planes, rows, scale=None):
    py_n, px_n = sizes
    columns = pieces[0].shape[1]
    shape = (2, 3, planes, py_n, px_n, rows, columns)
    sizes_ = [(l - f) * rows for _, _, f, l, _ in steps]
    hbm, vmem = pl.BlockSpec(memory_space=pltpu.HBM), pl.BlockSpec(memory_space=pltpu.VMEM)
    args = ([base] if base is not None else []) + ([mine] if scale is not None else []) + list(pieces)
    specs = ([hbm] if base is not None else []) + [vmem] * (len(args) - (base is not None))
    outs, out_specs = [jax.ShapeDtypeStruct(shape, jnp.float32)], [hbm]
    extra = []
    if scale is not None:
        outs.append(jax.ShapeDtypeStruct(mine.shape, jnp.float32))
        out_specs.append(vmem)
        extra = [pltpu.VMEM((py_n * px_n,) + mine.shape, jnp.float32)]
    done = pl.pallas_call(
        functools.partial(unpack_kernel, steps, sizes, planes, base is not None, scale),
        out_shape=outs,
        in_specs=specs,
        out_specs=out_specs,
        scratch_shapes=[pltpu.VMEM((max(s, 8), columns), jnp.float32) for s in sizes_]
        + [pltpu.SemaphoreType.DMA((len(steps),))]
        + extra,
        input_output_aliases={0: 0} if base is not None else {},
        compiler_params=pltpu.CompilerParams(vmem_limit_bytes=VMEM_LIMIT),
        cost_estimate=pl.CostEstimate(
            flops=0, bytes_accessed=6 * columns * sum(sizes_), transcendentals=0
        ),
        name="unpack",
    )(*args)
    return done if scale is not None else done[0]


def bin_kernel(state, shells, out):
    rows = 8
    width = shells.shape[2]
    low_ids = lax.broadcasted_iota(jnp.int32, (LOW, width), 0)
    high_ids = lax.broadcasted_iota(jnp.int32, (HIGH, width), 0)

    @pl.when(pl.program_id(0) == 0)
    def _():
        out[...] = jnp.zeros_like(out)

    def body(i, total):
        r0 = pl.multiple_of(i * rows, rows)
        energy = jnp.zeros((rows, width), jnp.float32)
        for c in range(2):
            for d in range(3):
                v = state[c, d, 0, pl.ds(r0, rows), :].astype(jnp.float32)
                energy = energy + v * v
        labels = shells[0, pl.ds(r0, rows), :]
        low, high = labels % LOW, labels // LOW
        upper = energy.astype(jnp.bfloat16).astype(jnp.float32)
        lower = energy - upper
        lhs, rhs = [], []
        for r in range(rows):
            at_low = jnp.broadcast_to(low[r : r + 1], (LOW, width)) == low_ids
            at_high = jnp.broadcast_to(high[r : r + 1], (HIGH, width)) == high_ids
            up = jnp.where(at_high, jnp.broadcast_to(upper[r : r + 1], (HIGH, width)), 0.0)
            lo = jnp.where(at_high, jnp.broadcast_to(lower[r : r + 1], (HIGH, width)), 0.0)
            lhs.append(jnp.concatenate([up.astype(jnp.bfloat16), lo.astype(jnp.bfloat16)], axis=0))
            rhs.append(jnp.where(at_low, 1.0, 0.0).astype(jnp.bfloat16))
        part = lax.dot_general(
            jnp.concatenate(lhs, axis=1),
            jnp.concatenate(rhs, axis=1),
            (((1,), (1,)), ((), ())),
            preferred_element_type=jnp.float32,
        )
        return total + part

    total = lax.fori_loop(0, shells.shape[1] // rows, body, jnp.zeros((2 * HIGH, LOW), jnp.float32))
    out[...] += total[:HIGH] + total[HIGH:]


def bin_energy(state, shells):
    _, _, planes, rows, width = state.shape
    return pl.pallas_call(
        bin_kernel,
        grid=(planes,),
        out_shape=jax.ShapeDtypeStruct((HIGH, LOW), jnp.float32),
        in_specs=[
            pl.BlockSpec((2, 3, 1, rows, width), lambda i: (0, 0, i, 0, 0)),
            pl.BlockSpec((1, rows, width), lambda i: (i, 0, 0)),
        ],
        out_specs=pl.BlockSpec((HIGH, LOW), lambda i: (0, 0)),
        cost_estimate=pl.CostEstimate(
            flops=4 * HIGH * LOW * planes * rows * width,
            bytes_accessed=16 * planes * rows * width,
            transcendentals=0,
        ),
        compiler_params=pltpu.CompilerParams(vmem_limit_bytes=VMEM_FIRST),
        name="bins",
    )(state, shells)


def steps_of(state, shells):
    py_n, px_n, slab_n = lax.axis_size("py"), lax.axis_size("px"), lax.axis_size("slab")
    sizes = (py_n, px_n)
    _, _, planes_all, rows, columns = state.shape
    planes = planes_all // py_n
    blocks = 6 * planes

    def send(x, step):
        a, b = step[:2]
        pairs = [
            (y * px_n + x_, partner(y, a, py_n) * px_n + partner(x_, b, px_n))
            for y in range(py_n)
            for x_ in range(px_n)
        ]
        return lax.ppermute(x, ("py", "px"), pairs)

    cut1, cut2 = max(1, blocks * CUTS[0] // 12), max(2, blocks * CUTS[1] // 12)
    fars = [[(a, b) for a in range(py_n)] for b in reversed(range(px_n // 2, px_n))]
    nears = [[(a, b) for a in range(py_n) if (a, b) != (0, 0)] for b in reversed(range(px_n // 2))]
    far = [s for g in fars for s in g]
    near = [s for g in nears for s in g]

    def part(steps, first, last, more=False):
        return [s + (first, last, more) for s in steps]

    stages = [part(far[:1], 0, cut1), part(fars[0][1:], 0, cut1), part(nears[0], 0, blocks)]
    stages += [part(far[py_n:], 0, cut1)] + [part(g, 0, blocks) for g in nears[1:]]
    early = []
    for steps in stages:
        packed = pack(state, None, steps, sizes, planes)
        early.append((steps, [send(x, s) for x, s in zip(packed, steps)]))
    own = pack(state, None, [(0, 0, 0, blocks, False)], sizes, planes)
    totals = bin_energy(state, shells)
    totals = totals.reshape(SHELLS // LANES, LANES)
    shift = 1 if is_power(slab_n) else slab_n
    if not is_power(slab_n):
        totals = lax.psum(totals, "slab")
    while shift < slab_n:
        totals = totals + lax.ppermute(totals, "slab", [(i, partner(i, shift, slab_n)) for i in range(slab_n)])
        shift *= 2
    mid = part(far, cut1, cut2, True) + part(near, blocks, blocks, True)
    late = part(far, cut2, blocks)
    packed = pack(state, totals, mid + late, sizes, planes)
    got = [send(x, s) for x, s in zip(packed, mid + late)]
    modes = slab_n * py_n * px_n * planes_all * rows * columns

    out = unpack(None, None, own, [(0, 0, 0, blocks, False)], sizes, planes, rows)
    for steps, pieces in early:
        out = unpack(out, None, pieces, steps, sizes, planes, rows)
    out, spectrum = unpack(
        out, totals, got[: len(mid)], mid, sizes, planes, rows, scale=0.5 * SHELLS / modes
    )
    out = unpack(out, None, got[len(mid) :], late, sizes, planes, rows)
    restored = out.reshape(2, 3, planes, py_n * px_n * rows, columns // px_n)
    return (restored, spectrum.reshape(SHELLS))


def solution(mesh):
    return jax.shard_map(
        steps_of,
        mesh=mesh,
        in_specs=(P(None, None, "slab", ("py", "px"), None), P("slab", ("py", "px"), None)),
        out_specs=(P(None, None, ("slab", "py"), None, "px"), P()),
        check_vma=False,
    )
```

```python
import functools

import jax
import jax.numpy as jnp
from jax import lax
from jax.experimental import pallas as pl
from jax.experimental.pallas import tpu as pltpu
from jax.sharding import PartitionSpec as P


SHELLS = 512
LOW = 32
HIGH = SHELLS // LOW
LANES = 256
CUTS = (7, 10)
VMEM_LIMIT = 40 * 1024 * 1024
VMEM_FIRST = 56 * 1024 * 1024


def is_power(n):
    return n & (n - 1) == 0


def partner(i, step, n, back=False):
    if is_power(n):
        return i ^ step
    return (i - step + n) % n if back else (i + step) % n


def joined(n):
    return 2 if n > 1 and is_power(n) else 1


def split3(x):
    a = x.astype(jnp.bfloat16)
    x = x - a.astype(jnp.float32)
    b = x.astype(jnp.bfloat16)
    return a, b, (x - b.astype(jnp.float32)).astype(jnp.bfloat16)


def whole_wait(ref, sem):
    pltpu.make_async_copy(ref, ref, sem).wait()


def pack_kernel(steps, sizes, planes, with_totals, *refs):
    (py_n, px_n), n = sizes, len(steps)
    refs = list(refs)
    state = refs.pop(0)
    totals = refs.pop(0) if with_totals else None
    outs, sems = refs[:n], refs[n]
    rows = state.shape[3]
    columns = outs[0].shape[1]
    me_y, me_x = lax.axis_index("py"), lax.axis_index("px")
    for k, (a, b, first, last, _) in enumerate(steps):
        to_y, to_x = partner(me_y, a, py_n), partner(me_x, b, px_n)
        across = pl.ds(pl.multiple_of(to_x * columns, columns), columns)
        for j in range(first, last):
            c, d, p = j // (3 * planes), j // planes % 3, j % planes
            pltpu.make_async_copy(
                state.at[c, d, to_y * planes + p, :, across],
                outs[k].at[pl.ds((j - first) * rows, rows), :],
                sems.at[k],
            ).start()
    if with_totals:
        t = totals[...]
        terms = split3(t) + (jnp.zeros_like(t).astype(jnp.bfloat16),)
        extra = jnp.concatenate([x.astype(jnp.float32) for x in terms], axis=0).astype(jnp.bfloat16)
        for k, (_, _, first, last, more) in enumerate(steps):
            if more:
                outs[k][pl.ds((last - first) * rows, 8), :] = extra
    for k, (_, _, first, last, _) in enumerate(steps):
        if first < last:
            whole_wait(outs[k].at[pl.ds(0, (last - first) * rows), :], sems.at[k])


def pack(state, totals, steps, sizes, planes):
    rows, columns = state.shape[3], state.shape[4] // sizes[1]
    shapes = [((l - f) * rows + (8 if more else 0), columns) for _, _, f, l, more in steps]
    vmem = pl.BlockSpec(memory_space=pltpu.VMEM)
    return pl.pallas_call(
        functools.partial(pack_kernel, steps, sizes, planes, totals is not None),
        out_shape=[jax.ShapeDtypeStruct(s, jnp.bfloat16) for s in shapes],
        in_specs=[pl.BlockSpec(memory_space=pltpu.HBM)] + ([vmem] if totals is not None else []),
        out_specs=[vmem] * len(steps),
        scratch_shapes=[pltpu.SemaphoreType.DMA((len(steps),))],
        compiler_params=pltpu.CompilerParams(
            vmem_limit_bytes=VMEM_FIRST if totals is None else VMEM_LIMIT
        ),
        cost_estimate=pl.CostEstimate(
            flops=0, bytes_accessed=sum(2 * r * c for r, c in shapes), transcendentals=0
        ),
        name="pack",
    )(state, *([totals] if totals is not None else []))


def unpack_kernel(steps, sizes, planes, with_base, scale, *refs):
    (py_n, px_n), n = sizes, len(steps)
    refs = list(refs)
    if with_base:
        refs.pop(0)
    mine = refs.pop(0) if scale is not None else None
    pieces = [refs.pop(0) for _ in range(n)]
    out = refs.pop(0)
    spectrum = refs.pop(0) if scale is not None else None
    wides, sems = refs[:n], refs[n]
    each = refs[n + 1] if scale is not None else None
    rows = out.shape[5]
    joint = joined(py_n)
    me_y, me_x = lax.axis_index("py"), lax.axis_index("px")
    for k, (a, b, first, last, more) in enumerate(steps):
        from_y, from_x = partner(me_y, a, py_n, True), partner(me_x, b, px_n, True)
        size = (last - first) * rows
        if first < last:
            wides[k][...] = pieces[k][pl.ds(0, size), :].astype(jnp.float32)
        for j in range(first, last):
            c, d, p = j // (3 * planes), j // planes % 3, j % planes
            pltpu.make_async_copy(
                wides[k].at[pl.ds((j - first) * rows, rows), :],
                out.at[c, d, p, from_y, from_x],
                sems.at[k],
            ).start()
        if more:
            extra = pieces[k][pl.ds(size, 8), :].astype(jnp.float32)
            each[from_y // joint * px_n + from_x] = (extra[0:2] + extra[2:4]) + extra[4:6]
    if scale is not None:
        a, b, c = [x.astype(jnp.float32) for x in split3(mine[...])]
        each[me_y // joint * px_n + me_x] = (a + b) + c
        total = each[0]
        for i in range(1, py_n // joint * px_n):
            total = total + each[i]
        spectrum[...] = total * scale
    for k, (_, _, first, last, _) in enumerate(steps):
        if first < last:
            whole_wait(wides[k], sems.at[k])


def unpack(base, mine, pieces, steps, sizes, planes, rows, scale=None):
    py_n, px_n = sizes
    columns = pieces[0].shape[1]
    shape = (2, 3, planes, py_n, px_n, rows, columns)
    sizes_ = [(l - f) * rows for _, _, f, l, _ in steps]
    hbm, vmem = pl.BlockSpec(memory_space=pltpu.HBM), pl.BlockSpec(memory_space=pltpu.VMEM)
    args = ([base] if base is not None else []) + ([mine] if scale is not None else []) + list(pieces)
    specs = ([hbm] if base is not None else []) + [vmem] * (len(args) - (base is not None))
    outs, out_specs = [jax.ShapeDtypeStruct(shape, jnp.float32)], [hbm]
    extra = []
    if scale is not None:
        outs.append(jax.ShapeDtypeStruct(mine.shape, jnp.float32))
        out_specs.append(vmem)
        extra = [pltpu.VMEM((py_n // joined(py_n) * px_n,) + mine.shape, jnp.float32)]
    done = pl.pallas_call(
        functools.partial(unpack_kernel, steps, sizes, planes, base is not None, scale),
        out_shape=outs,
        in_specs=specs,
        out_specs=out_specs,
        scratch_shapes=[pltpu.VMEM((max(s, 8), columns), jnp.float32) for s in sizes_]
        + [pltpu.SemaphoreType.DMA((len(steps),))]
        + extra,
        input_output_aliases={0: 0} if base is not None else {},
        compiler_params=pltpu.CompilerParams(vmem_limit_bytes=VMEM_LIMIT),
        cost_estimate=pl.CostEstimate(
            flops=0, bytes_accessed=6 * columns * sum(sizes_), transcendentals=0
        ),
        name="unpack",
    )(*args)
    return done if scale is not None else done[0]


def bin_kernel(state, shells, out):
    rows = 8
    width = shells.shape[2]
    low_ids = lax.broadcasted_iota(jnp.int32, (LOW, width), 0)
    high_ids = lax.broadcasted_iota(jnp.int32, (HIGH, width), 0)

    @pl.when(pl.program_id(0) == 0)
    def _():
        out[...] = jnp.zeros_like(out)

    def body(i, total):
        r0 = pl.multiple_of(i * rows, rows)
        energy = jnp.zeros((rows, width), jnp.float32)
        for c in range(2):
            for d in range(3):
                v = state[c, d, 0, pl.ds(r0, rows), :].astype(jnp.float32)
                energy = energy + v * v
        labels = shells[0, pl.ds(r0, rows), :]
        low, high = labels % LOW, labels // LOW
        upper = energy.astype(jnp.bfloat16).astype(jnp.float32)
        lower = energy - upper
        lhs, rhs = [], []
        for r in range(rows):
            at_low = jnp.broadcast_to(low[r : r + 1], (LOW, width)) == low_ids
            at_high = jnp.broadcast_to(high[r : r + 1], (HIGH, width)) == high_ids
            up = jnp.where(at_high, jnp.broadcast_to(upper[r : r + 1], (HIGH, width)), 0.0)
            lo = jnp.where(at_high, jnp.broadcast_to(lower[r : r + 1], (HIGH, width)), 0.0)
            lhs.append(jnp.concatenate([up.astype(jnp.bfloat16), lo.astype(jnp.bfloat16)], axis=0))
            rhs.append(jnp.where(at_low, 1.0, 0.0).astype(jnp.bfloat16))
        part = lax.dot_general(
            jnp.concatenate(lhs, axis=1),
            jnp.concatenate(rhs, axis=1),
            (((1,), (1,)), ((), ())),
            preferred_element_type=jnp.float32,
        )
        return total + part

    total = lax.fori_loop(0, shells.shape[1] // rows, body, jnp.zeros((2 * HIGH, LOW), jnp.float32))
    out[...] += total[:HIGH] + total[HIGH:]


def bin_energy(state, shells):
    _, _, planes, rows, width = state.shape
    return pl.pallas_call(
        bin_kernel,
        grid=(planes,),
        out_shape=jax.ShapeDtypeStruct((HIGH, LOW), jnp.float32),
        in_specs=[
            pl.BlockSpec((2, 3, 1, rows, width), lambda i: (0, 0, i, 0, 0)),
            pl.BlockSpec((1, rows, width), lambda i: (i, 0, 0)),
        ],
        out_specs=pl.BlockSpec((HIGH, LOW), lambda i: (0, 0)),
        cost_estimate=pl.CostEstimate(
            flops=4 * HIGH * LOW * planes * rows * width,
            bytes_accessed=16 * planes * rows * width,
            transcendentals=0,
        ),
        compiler_params=pltpu.CompilerParams(vmem_limit_bytes=VMEM_FIRST),
        name="bins",
    )(state, shells)


def steps_of(state, shells):
    py_n, px_n, slab_n = lax.axis_size("py"), lax.axis_size("px"), lax.axis_size("slab")
    sizes = (py_n, px_n)
    _, _, planes_all, rows, columns = state.shape
    planes = planes_all // py_n
    blocks = 6 * planes

    def send(x, step):
        a, b = step[:2]
        pairs = [
            (y * px_n + x_, partner(y, a, py_n) * px_n + partner(x_, b, px_n))
            for y in range(py_n)
            for x_ in range(px_n)
        ]
        return lax.ppermute(x, ("py", "px"), pairs)

    cut1, cut2 = max(1, blocks * CUTS[0] // 12), max(2, blocks * CUTS[1] // 12)
    fars = [[(a, b) for a in range(py_n)] for b in reversed(range(px_n // 2, px_n))]
    nears = [[(a, b) for a in range(py_n) if (a, b) != (0, 0)] for b in reversed(range(px_n // 2))]
    far = [s for g in fars for s in g]
    near = [s for g in nears for s in g]

    def part(steps, first, last, more=False):
        return [s + (first, last, more) for s in steps]

    stages = [part(far[:1], 0, cut1), part(fars[0][1:], 0, cut1), part(nears[0], 0, blocks)]
    stages += [part(far[py_n:], 0, cut1)] + [part(g, 0, blocks) for g in nears[1:]]
    early = []
    for steps in stages:
        packed = pack(state, None, steps, sizes, planes)
        early.append((steps, [send(x, s) for x, s in zip(packed, steps)]))
    own = pack(state, None, [(0, 0, 0, blocks, False)], sizes, planes)
    totals = bin_energy(state, shells)
    totals = totals.reshape(SHELLS // LANES, LANES)
    joint = joined(py_n)
    for axis, n, bits in (("slab", slab_n, slab_n.bit_length() - 1), ("py", py_n, joint - 1)):
        if axis == "slab" and not is_power(n):
            totals = lax.psum(totals, axis)
            continue
        for bit in range(bits):
            pairs = [(i, i ^ (1 << bit)) for i in range(n)]
            totals = totals + lax.ppermute(totals, axis, pairs)
    mid = [s + (cut1, cut2, s[0] % joint == 0) for s in far]
    mid += part([s for s in near if s[0] % joint == 0], blocks, blocks, True)
    late = part([(a, b) for b in range(px_n // 2, px_n) for a in [*range(py_n // 2, py_n), *range(py_n // 2)]], cut2, blocks)
    packed = pack(state, totals, mid + late, sizes, planes)
    got = [send(x, s) for x, s in zip(packed, mid + late)]
    modes = slab_n * py_n * px_n * planes_all * rows * columns

    out = unpack(None, None, own, [(0, 0, 0, blocks, False)], sizes, planes, rows)
    for steps, pieces in early:
        out = unpack(out, None, pieces, steps, sizes, planes, rows)
    out, spectrum = unpack(
        out, totals, got[: len(mid)], mid, sizes, planes, rows, scale=0.5 * SHELLS / modes
    )
    out = unpack(out, None, got[len(mid) :], late, sizes, planes, rows)
    restored = out.reshape(2, 3, planes, py_n * px_n * rows, columns // px_n)
    return (restored, spectrum.reshape(SHELLS))


def solution(mesh):
    return jax.shard_map(
        steps_of,
        mesh=mesh,
        in_specs=(P(None, None, "slab", ("py", "px"), None), P("slab", ("py", "px"), None)),
        out_specs=(P(None, None, ("slab", "py"), None, "px"), P()),
        check_vma=False,
    )
```

```python
import functools

import jax
import jax.numpy as jnp
from jax import lax
from jax.experimental import pallas as pl
from jax.experimental.pallas import tpu as pltpu
from jax.sharding import PartitionSpec as P


SHELLS = 512
LOW = 32
HIGH = SHELLS // LOW
LANES = 256
CUTS = (7, 10)
VMEM_LIMIT = 40 * 1024 * 1024
VMEM_FIRST = 56 * 1024 * 1024


def is_power(n):
    return n & (n - 1) == 0


def partner(i, step, n, back=False):
    if is_power(n):
        return i ^ step
    return (i - step + n) % n if back else (i + step) % n


def add_groups(totals, slab_n, py_n):
    if not (is_power(slab_n) and is_power(py_n)):
        return lax.psum(totals, ("slab", "py"))
    bits = lambda n: [1 << k for k in range(n.bit_length() - 1)]
    swaps = [(min(1, slab_n - 1), p) for p in bits(py_n)[1:]]
    swaps += [(s, 0) for s in bits(slab_n)] + [(0, p) for p in bits(py_n)[:1]]
    for s, p in swaps:
        pairs = [
            (i * py_n + j, (i ^ s) * py_n + (j ^ p)) for i in range(slab_n) for j in range(py_n)
        ]
        totals = totals + lax.ppermute(totals, ("slab", "py"), pairs)
    return totals


def split3(x):
    a = x.astype(jnp.bfloat16)
    x = x - a.astype(jnp.float32)
    b = x.astype(jnp.bfloat16)
    return a, b, (x - b.astype(jnp.float32)).astype(jnp.bfloat16)


def whole_wait(ref, sem):
    pltpu.make_async_copy(ref, ref, sem).wait()


def pack_kernel(steps, sizes, planes, with_totals, *refs):
    (py_n, px_n), n = sizes, len(steps)
    refs = list(refs)
    state = refs.pop(0)
    totals = refs.pop(0) if with_totals else None
    outs, sems = refs[:n], refs[n]
    rows = state.shape[3]
    columns = outs[0].shape[1]
    me_y, me_x = lax.axis_index("py"), lax.axis_index("px")
    for k, (a, b, first, last, _) in enumerate(steps):
        to_y, to_x = partner(me_y, a, py_n), partner(me_x, b, px_n)
        across = pl.ds(pl.multiple_of(to_x * columns, columns), columns)
        for j in range(first, last):
            c, d, p = j // (3 * planes), j // planes % 3, j % planes
            pltpu.make_async_copy(
                state.at[c, d, to_y * planes + p, :, across],
                outs[k].at[pl.ds((j - first) * rows, rows), :],
                sems.at[k],
            ).start()
    if with_totals:
        t = totals[...]
        terms = split3(t) + (jnp.zeros_like(t).astype(jnp.bfloat16),)
        extra = jnp.concatenate([x.astype(jnp.float32) for x in terms], axis=0).astype(jnp.bfloat16)
        for k, (_, _, first, last, more) in enumerate(steps):
            if more:
                outs[k][pl.ds((last - first) * rows, 8), :] = extra
    for k, (_, _, first, last, _) in enumerate(steps):
        if first < last:
            whole_wait(outs[k].at[pl.ds(0, (last - first) * rows), :], sems.at[k])


def pack(state, totals, steps, sizes, planes):
    rows, columns = state.shape[3], state.shape[4] // sizes[1]
    shapes = [((l - f) * rows + (8 if more else 0), columns) for _, _, f, l, more in steps]
    vmem = pl.BlockSpec(memory_space=pltpu.VMEM)
    return pl.pallas_call(
        functools.partial(pack_kernel, steps, sizes, planes, totals is not None),
        out_shape=[jax.ShapeDtypeStruct(s, jnp.bfloat16) for s in shapes],
        in_specs=[pl.BlockSpec(memory_space=pltpu.HBM)] + ([vmem] if totals is not None else []),
        out_specs=[vmem] * len(steps),
        scratch_shapes=[pltpu.SemaphoreType.DMA((len(steps),))],
        compiler_params=pltpu.CompilerParams(
            vmem_limit_bytes=VMEM_FIRST if totals is None else VMEM_LIMIT
        ),
        cost_estimate=pl.CostEstimate(
            flops=0, bytes_accessed=sum(2 * r * c for r, c in shapes), transcendentals=0
        ),
        name="pack",
    )(state, *([totals] if totals is not None else []))


def unpack_kernel(steps, sizes, planes, with_base, scale, *refs):
    (py_n, px_n), n = sizes, len(steps)
    refs = list(refs)
    if with_base:
        refs.pop(0)
    mine = refs.pop(0) if scale is not None else None
    pieces = [refs.pop(0) for _ in range(n)]
    out = refs.pop(0)
    spectrum = refs.pop(0) if scale is not None else None
    wides, sems = refs[:n], refs[n]
    each = refs[n + 1] if scale is not None else None
    rows = out.shape[5]
    me_y, me_x = lax.axis_index("py"), lax.axis_index("px")
    for k, (a, b, first, last, more) in enumerate(steps):
        from_y, from_x = partner(me_y, a, py_n, True), partner(me_x, b, px_n, True)
        size = (last - first) * rows
        if first < last:
            wides[k][...] = pieces[k][pl.ds(0, size), :].astype(jnp.float32)
        for j in range(first, last):
            c, d, p = j // (3 * planes), j // planes % 3, j % planes
            pltpu.make_async_copy(
                wides[k].at[pl.ds((j - first) * rows, rows), :],
                out.at[c, d, p, from_y, from_x],
                sems.at[k],
            ).start()
        if more:
            extra = pieces[k][pl.ds(size, 8), :].astype(jnp.float32)
            each[from_x] = (extra[0:2] + extra[2:4]) + extra[4:6]
    if scale is not None:
        a, b, c = [x.astype(jnp.float32) for x in split3(mine[...])]
        each[me_x] = (a + b) + c
        total = each[0]
        for i in range(1, px_n):
            total = total + each[i]
        spectrum[...] = total * scale
    for k, (_, _, first, last, _) in enumerate(steps):
        if first < last:
            whole_wait(wides[k], sems.at[k])


def unpack(base, mine, pieces, steps, sizes, planes, rows, scale=None):
    py_n, px_n = sizes
    columns = pieces[0].shape[1]
    shape = (2, 3, planes, py_n, px_n, rows, columns)
    sizes_ = [(l - f) * rows for _, _, f, l, _ in steps]
    hbm, vmem = pl.BlockSpec(memory_space=pltpu.HBM), pl.BlockSpec(memory_space=pltpu.VMEM)
    args = ([base] if base is not None else []) + ([mine] if scale is not None else []) + list(pieces)
    specs = ([hbm] if base is not None else []) + [vmem] * (len(args) - (base is not None))
    outs, out_specs = [jax.ShapeDtypeStruct(shape, jnp.float32)], [hbm]
    extra = []
    if scale is not None:
        outs.append(jax.ShapeDtypeStruct(mine.shape, jnp.float32))
        out_specs.append(vmem)
        extra = [pltpu.VMEM((px_n,) + mine.shape, jnp.float32)]
    done = pl.pallas_call(
        functools.partial(unpack_kernel, steps, sizes, planes, base is not None, scale),
        out_shape=outs,
        in_specs=specs,
        out_specs=out_specs,
        scratch_shapes=[pltpu.VMEM((max(s, 8), columns), jnp.float32) for s in sizes_]
        + [pltpu.SemaphoreType.DMA((len(steps),))]
        + extra,
        input_output_aliases={0: 0} if base is not None else {},
        compiler_params=pltpu.CompilerParams(vmem_limit_bytes=VMEM_LIMIT),
        cost_estimate=pl.CostEstimate(
            flops=0, bytes_accessed=6 * columns * sum(sizes_), transcendentals=0
        ),
        name="unpack",
    )(*args)
    return done if scale is not None else done[0]


def bin_kernel(state, shells, out):
    rows = 8
    width = shells.shape[2]
    low_ids = lax.broadcasted_iota(jnp.int32, (LOW, width), 0)
    high_ids = lax.broadcasted_iota(jnp.int32, (HIGH, width), 0)

    @pl.when(pl.program_id(0) == 0)
    def _():
        out[...] = jnp.zeros_like(out)

    def body(i, total):
        r0 = pl.multiple_of(i * rows, rows)
        energy = jnp.zeros((rows, width), jnp.float32)
        for c in range(2):
            for d in range(3):
                v = state[c, d, 0, pl.ds(r0, rows), :].astype(jnp.float32)
                energy = energy + v * v
        labels = shells[0, pl.ds(r0, rows), :]
        low, high = labels % LOW, labels // LOW
        upper = energy.astype(jnp.bfloat16).astype(jnp.float32)
        lower = energy - upper
        lhs, rhs = [], []
        for r in range(rows):
            at_low = jnp.broadcast_to(low[r : r + 1], (LOW, width)) == low_ids
            at_high = jnp.broadcast_to(high[r : r + 1], (HIGH, width)) == high_ids
            up = jnp.where(at_high, jnp.broadcast_to(upper[r : r + 1], (HIGH, width)), 0.0)
            lo = jnp.where(at_high, jnp.broadcast_to(lower[r : r + 1], (HIGH, width)), 0.0)
            lhs.append(jnp.concatenate([up.astype(jnp.bfloat16), lo.astype(jnp.bfloat16)], axis=0))
            rhs.append(jnp.where(at_low, 1.0, 0.0).astype(jnp.bfloat16))
        part = lax.dot_general(
            jnp.concatenate(lhs, axis=1),
            jnp.concatenate(rhs, axis=1),
            (((1,), (1,)), ((), ())),
            preferred_element_type=jnp.float32,
        )
        return total + part

    total = lax.fori_loop(0, shells.shape[1] // rows, body, jnp.zeros((2 * HIGH, LOW), jnp.float32))
    out[...] += total[:HIGH] + total[HIGH:]


def bin_energy(state, shells):
    _, _, planes, rows, width = state.shape
    return pl.pallas_call(
        bin_kernel,
        grid=(planes,),
        out_shape=jax.ShapeDtypeStruct((HIGH, LOW), jnp.float32),
        in_specs=[
            pl.BlockSpec((2, 3, 1, rows, width), lambda i: (0, 0, i, 0, 0)),
            pl.BlockSpec((1, rows, width), lambda i: (i, 0, 0)),
        ],
        out_specs=pl.BlockSpec((HIGH, LOW), lambda i: (0, 0)),
        cost_estimate=pl.CostEstimate(
            flops=4 * HIGH * LOW * planes * rows * width,
            bytes_accessed=16 * planes * rows * width,
            transcendentals=0,
        ),
        compiler_params=pltpu.CompilerParams(vmem_limit_bytes=VMEM_FIRST),
        name="bins",
    )(state, shells)


def steps_of(state, shells):
    py_n, px_n, slab_n = lax.axis_size("py"), lax.axis_size("px"), lax.axis_size("slab")
    sizes = (py_n, px_n)
    _, _, planes_all, rows, columns = state.shape
    planes = planes_all // py_n
    blocks = 6 * planes

    def send(x, step):
        a, b = step[:2]
        pairs = [
            (y * px_n + x_, partner(y, a, py_n) * px_n + partner(x_, b, px_n))
            for y in range(py_n)
            for x_ in range(px_n)
        ]
        return lax.ppermute(x, ("py", "px"), pairs)

    cut1, cut2 = max(1, blocks * CUTS[0] // 12), max(2, blocks * CUTS[1] // 12)
    fars = [[(a, b) for a in range(py_n)] for b in reversed(range(px_n // 2, px_n))]
    nears = [[(a, b) for a in range(py_n) if (a, b) != (0, 0)] for b in reversed(range(px_n // 2))]
    far = [s for g in fars for s in g]
    near = [s for g in nears for s in g]

    def part(steps, first, last, more=False):
        return [s + (first, last, more) for s in steps]

    stages = [part(far[:1], 0, cut1), part(fars[0][1:], 0, cut1), part(nears[0], 0, blocks)]
    stages += [part(far[py_n:], 0, cut1)] + [part(g, 0, blocks) for g in nears[1:]]
    early = []
    for steps in stages:
        packed = pack(state, None, steps, sizes, planes)
        early.append((steps, [send(x, s) for x, s in zip(packed, steps)]))
    own = pack(state, None, [(0, 0, 0, blocks, False)], sizes, planes)
    totals = bin_energy(state, shells)
    totals = totals.reshape(SHELLS // LANES, LANES)
    totals = add_groups(totals, slab_n, py_n)
    mid = [s + (cut1, cut2, s[0] == 0) for s in far]
    mid += part([s for s in near if s[0] == 0], blocks, blocks, True)
    late = part([(a, b) for b in range(px_n // 2, px_n) for a in [*range(py_n // 2, py_n), *range(py_n // 2)]], cut2, blocks)
    packed = pack(state, totals, mid + late, sizes, planes)
    got = [send(x, s) for x, s in zip(packed, mid + late)]
    modes = slab_n * py_n * px_n * planes_all * rows * columns

    out = unpack(None, None, own, [(0, 0, 0, blocks, False)], sizes, planes, rows)
    for steps, pieces in early:
        out = unpack(out, None, pieces, steps, sizes, planes, rows)
    out, spectrum = unpack(
        out, totals, got[: len(mid)], mid, sizes, planes, rows, scale=0.5 * SHELLS / modes
    )
    got, start = got[len(mid) :], 0
    for stop in (len(late) // 2, len(late) * 3 // 4, len(late)):
        out = unpack(out, None, got[start:stop], late[start:stop], sizes, planes, rows)
        start = stop
    restored = out.reshape(2, 3, planes, py_n * px_n * rows, columns // px_n)
    return (restored, spectrum.reshape(SHELLS))


def solution(mesh):
    return jax.shard_map(
        steps_of,
        mesh=mesh,
        in_specs=(P(None, None, "slab", ("py", "px"), None), P("slab", ("py", "px"), None)),
        out_specs=(P(None, None, ("slab", "py"), None, "px"), P()),
        check_vma=False,
    )
```

```python
import functools

import jax
import jax.numpy as jnp
from jax import lax
from jax.experimental import pallas as pl
from jax.experimental.pallas import tpu as pltpu
from jax.sharding import PartitionSpec as P


SHELLS = 512
LOW = 32
HIGH = SHELLS // LOW
LANES = 256
CUTS = (7, 10)
VMEM_LIMIT = 16 * 1024 * 1024
VMEM_FIRST = 53 * 1024 * 1024
VMEM_EARLY = 45 * 1024 * 1024


def is_power(n):
    return n & (n - 1) == 0


def partner(i, step, n, back=False):
    if is_power(n):
        return i ^ step
    return (i - step + n) % n if back else (i + step) % n


def add_groups(totals, slab_n, py_n):
    if not (is_power(slab_n) and is_power(py_n)):
        return lax.psum(totals, ("slab", "py"))
    bits = lambda n: [1 << k for k in range(n.bit_length() - 1)]
    swaps = [(min(1, slab_n - 1), p) for p in bits(py_n)[1:]]
    swaps += [(s, 0) for s in bits(slab_n)] + [(0, p) for p in bits(py_n)[:1]]
    for s, p in swaps:
        pairs = [
            (i * py_n + j, (i ^ s) * py_n + (j ^ p)) for i in range(slab_n) for j in range(py_n)
        ]
        totals = totals + lax.ppermute(totals, ("slab", "py"), pairs)
    return totals


def split3(x):
    a = x.astype(jnp.bfloat16)
    x = x - a.astype(jnp.float32)
    b = x.astype(jnp.bfloat16)
    return a, b, (x - b.astype(jnp.float32)).astype(jnp.bfloat16)


def whole_wait(ref, sem):
    pltpu.make_async_copy(ref, ref, sem).wait()


def pack_kernel(steps, sizes, planes, with_totals, *refs):
    (py_n, px_n), n = sizes, len(steps)
    refs = list(refs)
    state = refs.pop(0)
    totals = refs.pop(0) if with_totals else None
    outs, sems = refs[:n], refs[n]
    rows = state.shape[3]
    columns = outs[0].shape[1]
    me_y, me_x = lax.axis_index("py"), lax.axis_index("px")
    for k, (a, b, first, last, _) in enumerate(steps):
        to_y, to_x = partner(me_y, a, py_n), partner(me_x, b, px_n)
        across = pl.ds(pl.multiple_of(to_x * columns, columns), columns)
        for j in range(first, last):
            c, d, p = j // (3 * planes), j // planes % 3, j % planes
            pltpu.make_async_copy(
                state.at[c, d, to_y * planes + p, :, across],
                outs[k].at[pl.ds((j - first) * rows, rows), :],
                sems.at[k],
            ).start()
    if with_totals:
        t = totals[...]
        terms = split3(t) + (jnp.zeros_like(t).astype(jnp.bfloat16),)
        extra = jnp.concatenate([x.astype(jnp.float32) for x in terms], axis=0).astype(jnp.bfloat16)
        for k, (_, _, first, last, more) in enumerate(steps):
            if more:
                outs[k][pl.ds((last - first) * rows, 8), :] = extra
    for k, (_, _, first, last, _) in enumerate(steps):
        if first < last:
            whole_wait(outs[k].at[pl.ds(0, (last - first) * rows), :], sems.at[k])


def pack(state, totals, steps, sizes, planes, limit=VMEM_LIMIT):
    rows, columns = state.shape[3], state.shape[4] // sizes[1]
    shapes = [((l - f) * rows + (8 if more else 0), columns) for _, _, f, l, more in steps]
    vmem = pl.BlockSpec(memory_space=pltpu.VMEM)
    return pl.pallas_call(
        functools.partial(pack_kernel, steps, sizes, planes, totals is not None),
        out_shape=[jax.ShapeDtypeStruct(s, jnp.bfloat16) for s in shapes],
        in_specs=[pl.BlockSpec(memory_space=pltpu.HBM)] + ([vmem] if totals is not None else []),
        out_specs=[vmem] * len(steps),
        scratch_shapes=[pltpu.SemaphoreType.DMA((len(steps),))],
        compiler_params=pltpu.CompilerParams(vmem_limit_bytes=limit),
        cost_estimate=pl.CostEstimate(
            flops=0, bytes_accessed=sum(2 * r * c for r, c in shapes), transcendentals=0
        ),
        name="pack",
    )(state, *([totals] if totals is not None else []))


def unpack_kernel(steps, sizes, planes, with_base, scale, *refs):
    (py_n, px_n), n = sizes, len(steps)
    refs = list(refs)
    if with_base:
        refs.pop(0)
    mine = refs.pop(0) if scale is not None else None
    pieces = [refs.pop(0) for _ in range(n)]
    out = refs.pop(0)
    spectrum = refs.pop(0) if scale is not None else None
    wides, sems = refs[:n], refs[n]
    each = refs[n + 1] if scale is not None else None
    rows = out.shape[5]
    me_y, me_x = lax.axis_index("py"), lax.axis_index("px")
    for k, (a, b, first, last, more) in enumerate(steps):
        from_y, from_x = partner(me_y, a, py_n, True), partner(me_x, b, px_n, True)
        size = (last - first) * rows
        if first < last:
            wides[k][...] = pieces[k][pl.ds(0, size), :].astype(jnp.float32)
        for j in range(first, last):
            c, d, p = j // (3 * planes), j // planes % 3, j % planes
            pltpu.make_async_copy(
                wides[k].at[pl.ds((j - first) * rows, rows), :],
                out.at[c, d, p, from_y, from_x],
                sems.at[k],
            ).start()
        if more:
            extra = pieces[k][pl.ds(size, 8), :].astype(jnp.float32)
            each[from_x] = (extra[0:2] + extra[2:4]) + extra[4:6]
    if scale is not None:
        a, b, c = [x.astype(jnp.float32) for x in split3(mine[...])]
        each[me_x] = (a + b) + c
        total = each[0]
        for i in range(1, px_n):
            total = total + each[i]
        spectrum[...] = total * scale
    for k, (_, _, first, last, _) in enumerate(steps):
        if first < last:
            whole_wait(wides[k], sems.at[k])


def unpack(base, mine, pieces, steps, sizes, planes, rows, scale=None):
    py_n, px_n = sizes
    columns = pieces[0].shape[1]
    shape = (2, 3, planes, py_n, px_n, rows, columns)
    sizes_ = [(l - f) * rows for _, _, f, l, _ in steps]
    hbm, vmem = pl.BlockSpec(memory_space=pltpu.HBM), pl.BlockSpec(memory_space=pltpu.VMEM)
    args = ([base] if base is not None else []) + ([mine] if scale is not None else []) + list(pieces)
    specs = ([hbm] if base is not None else []) + [vmem] * (len(args) - (base is not None))
    outs, out_specs = [jax.ShapeDtypeStruct(shape, jnp.float32)], [hbm]
    extra = []
    if scale is not None:
        outs.append(jax.ShapeDtypeStruct(mine.shape, jnp.float32))
        out_specs.append(vmem)
        extra = [pltpu.VMEM((px_n,) + mine.shape, jnp.float32)]
    done = pl.pallas_call(
        functools.partial(unpack_kernel, steps, sizes, planes, base is not None, scale),
        out_shape=outs,
        in_specs=specs,
        out_specs=out_specs,
        scratch_shapes=[pltpu.VMEM((max(s, 8), columns), jnp.float32) for s in sizes_]
        + [pltpu.SemaphoreType.DMA((len(steps),))]
        + extra,
        input_output_aliases={0: 0} if base is not None else {},
        compiler_params=pltpu.CompilerParams(vmem_limit_bytes=VMEM_LIMIT),
        cost_estimate=pl.CostEstimate(
            flops=0, bytes_accessed=6 * columns * sum(sizes_), transcendentals=0
        ),
        name="unpack",
    )(*args)
    return done if scale is not None else done[0]


def bin_kernel(state, shells, out, sums):
    rows = 8
    width = shells.shape[2]
    low_ids = lax.broadcasted_iota(jnp.int32, (LOW, width), 0)
    high_ids = lax.broadcasted_iota(jnp.int32, (HIGH, width), 0)

    @pl.when(pl.program_id(0) == 0)
    def _():
        sums[...] = jnp.zeros_like(sums)

    def body(i, total):
        r0 = pl.multiple_of(i * rows, rows)
        energy = jnp.zeros((rows, width), jnp.float32)
        for c in range(2):
            for d in range(3):
                v = state[c, d, 0, pl.ds(r0, rows), :].astype(jnp.float32)
                energy = energy + v * v
        labels = shells[0, pl.ds(r0, rows), :]
        low, high = labels % LOW, labels // LOW
        upper = energy.astype(jnp.bfloat16).astype(jnp.float32)
        lower = energy - upper
        lhs, rhs = [], []
        for r in range(rows):
            at_low = jnp.broadcast_to(low[r : r + 1], (LOW, width)) == low_ids
            at_high = jnp.broadcast_to(high[r : r + 1], (HIGH, width)) == high_ids
            up = jnp.where(at_high, jnp.broadcast_to(upper[r : r + 1], (HIGH, width)), 0.0)
            lo = jnp.where(at_high, jnp.broadcast_to(lower[r : r + 1], (HIGH, width)), 0.0)
            lhs.append(jnp.concatenate([up.astype(jnp.bfloat16), lo.astype(jnp.bfloat16)], axis=0))
            rhs.append(jnp.where(at_low, 1.0, 0.0).astype(jnp.bfloat16))
        part = lax.dot_general(
            jnp.concatenate(lhs, axis=1),
            jnp.concatenate(rhs, axis=1),
            (((1,), (1,)), ((), ())),
            preferred_element_type=jnp.float32,
        )
        return total + part

    total = lax.fori_loop(0, shells.shape[1] // rows, body, jnp.zeros((2 * HIGH, LOW), jnp.float32))
    sums[...] += total[:HIGH] + total[HIGH:]

    @pl.when(pl.program_id(0) == pl.num_programs(0) - 1)
    def _():
        per_row = LANES // LOW
        for k in range(HIGH):
            r, g = k // per_row, k % per_row
            out[r : r + 1, g * LOW : (g + 1) * LOW] = sums[k : k + 1, :]


def bin_energy(state, shells, limit):
    _, _, planes, rows, width = state.shape
    return pl.pallas_call(
        bin_kernel,
        grid=(planes,),
        out_shape=jax.ShapeDtypeStruct((SHELLS // LANES, LANES), jnp.float32),
        in_specs=[
            pl.BlockSpec((2, 3, 1, rows, width), lambda i: (0, 0, i, 0, 0)),
            pl.BlockSpec((1, rows, width), lambda i: (i, 0, 0)),
        ],
        out_specs=pl.BlockSpec((SHELLS // LANES, LANES), lambda i: (0, 0)),
        scratch_shapes=[pltpu.VMEM((HIGH, LOW), jnp.float32)],
        cost_estimate=pl.CostEstimate(
            flops=4 * HIGH * LOW * planes * rows * width,
            bytes_accessed=16 * planes * rows * width,
            transcendentals=0,
        ),
        compiler_params=pltpu.CompilerParams(vmem_limit_bytes=limit),
        name="bins",
    )(state, shells)


def steps_of(state, shells):
    py_n, px_n, slab_n = lax.axis_size("py"), lax.axis_size("px"), lax.axis_size("slab")
    sizes = (py_n, px_n)
    _, _, planes_all, rows, columns = state.shape
    planes = planes_all // py_n
    blocks = 6 * planes

    def send(x, step):
        a, b = step[:2]
        pairs = [
            (y * px_n + x_, partner(y, a, py_n) * px_n + partner(x_, b, px_n))
            for y in range(py_n)
            for x_ in range(px_n)
        ]
        return lax.ppermute(x, ("py", "px"), pairs)

    cut1, cut2 = max(1, blocks * CUTS[0] // 12), max(2, blocks * CUTS[1] // 12)
    fars = [[(a, b) for a in range(py_n)] for b in reversed(range(px_n // 2, px_n))]
    nears = [[(a, b) for a in range(py_n) if (a, b) != (0, 0)] for b in reversed(range(px_n // 2))]
    far = [s for g in fars for s in g]
    near = [s for g in nears for s in g]

    def part(steps, first, last, more=False):
        return [s + (first, last, more) for s in steps]

    stages = [part(far[:1], 0, cut1), part(fars[0][1:], 0, cut1), part(nears[0], 0, blocks)]
    stages += [part(far[py_n:], 0, cut1)] + [part(g, 0, blocks) for g in nears[1:]]
    early = []
    for n, steps in enumerate(stages):
        limit = VMEM_FIRST if n == 0 else VMEM_EARLY
        packed = pack(state, None, steps, sizes, planes, limit)
        early.append((steps, [send(x, s) for x, s in zip(packed, steps)]))
    own = pack(state, None, [(0, 0, 0, blocks, False)], sizes, planes)
    totals = bin_energy(state, shells, limit)
    totals = add_groups(totals, slab_n, py_n)
    mid = [s + (cut1, cut2, s[0] == 0) for s in far]
    mid += part([s for s in near if s[0] == 0], blocks, blocks, True)
    late = part([(a, b) for b in range(px_n // 2, px_n) for a in [*range(py_n // 2, py_n), *range(py_n // 2)]], cut2, blocks)
    if len(late) > py_n:
        late[py_n - 1], late[py_n] = late[py_n], late[py_n - 1]
    packed = pack(state, totals, mid + late, sizes, planes)
    got = [send(x, s) for x, s in zip(packed, mid + late)]
    modes = slab_n * py_n * px_n * planes_all * rows * columns

    out = unpack(None, None, own, [(0, 0, 0, blocks, False)], sizes, planes, rows)
    for steps, pieces in early:
        out = unpack(out, None, pieces, steps, sizes, planes, rows)
    out, spectrum = unpack(
        out, totals, got[: len(mid)], mid, sizes, planes, rows, scale=0.5 * SHELLS / modes
    )
    got, start = got[len(mid) :], 0
    for stop in (len(late) // 2, len(late) * 7 // 8, len(late)):
        out = unpack(out, None, got[start:stop], late[start:stop], sizes, planes, rows)
        start = stop
    restored = out.reshape(2, 3, planes, py_n * px_n * rows, columns // px_n)
    return (restored, spectrum.reshape(SHELLS))


def solution(mesh):
    return jax.shard_map(
        steps_of,
        mesh=mesh,
        in_specs=(P(None, None, "slab", ("py", "px"), None), P("slab", ("py", "px"), None)),
        out_specs=(P(None, None, ("slab", "py"), None, "px"), P()),
        check_vma=False,
    )
```
